32 devices in a mesh: expert: 16 (over z, y, x), dp: 2 (over core).
Axes of the slice: x: 2, y: 2, z: 4, core: 2. Of those that a mesh axis runs over, the one named last changes fastest.
Arguments:
- tokens: bfloat16 [4096, 1440], P(('expert', 'dp')), may hold values from -6 to 6
- cotangent: bfloat16 [4096, 1440], P(('expert', 'dp')), may hold values from -0.3984375 to 0.3984375
- expert_ids: int32 [4096, 4], P(('expert', 'dp')), may hold values from 0 to 15, all different within a row; in each aligned block of 128 rows (0 to 127, 128 to 255, ...) at most 48 rows name the same one
- gate_weights: float32 [4096, 4], P(('expert', 'dp')), may hold values from 0.05 to 1
- w_gate: bfloat16 [16, 1440, 1440], P('expert', 'dp'), may hold values from -0.15625 to 0.15625
- w_up: bfloat16 [16, 1440, 1440], P('expert', 'dp'), may hold values from -0.15625 to 0.15625
- w_down: bfloat16 [16, 1440, 1440], P('expert', 'dp'), may hold values from -0.15625 to 0.15625
Outputs:
- mixed: bfloat16 [4096, 1440], P(('expert', 'dp'))
- grad_gate: bfloat16 [16, 1440, 1440], P('expert', 'dp')
- grad_up: bfloat16 [16, 1440, 1440], P('expert', 'dp')
- grad_down: bfloat16 [16, 1440, 1440], P('expert', 'dp')
The draws below stay inside these ranges and needn't reach their ends.
Inputs may be any that keep to these rules, and one draw needn't show every extreme that they name: `expert_ids`: each row names 4 different experts. Within the rows of one device no expert is named more than 48 times, a bound that some block reaches.
All inputs are finite; a program needn't handle non-finite values.
Results may differ from the reference program's by a relative error of at most 0.013.
Values may be sent and summed in bfloat16 or wider, within the bound.
A program may use at most 128 MiB of HBM per device.

```python
import math
import jax
import jax.numpy as jnp
import numpy as np
from jax import lax

D = 1440
FH = 1440
TOPK = 4
TOK_DEV = 128
CAP = 512
EXPERTS = 16
SLOT = 48
TOKENS = 4096
N_EXPERT = 16
N_DP = 2


def shard_levels(key, dims, pieces, smallest, high):
    level = 1.0
    for dim, shards_of in pieces:
        draws = jax.random.uniform(jax.random.fold_in(jax.random.fold_in(key, 6), dim), (shards_of,), jnp.float32, smallest / len(pieces), high / len(pieces))
        level = level * jnp.repeat(jnp.exp(draws), dims[dim] // shards_of).reshape((-1,) + (1,) * (len(dims) - 1 - dim))
    return level


def routed_block(stream_key, own, number, rows, number_of, top, reach, skew):
    ranking = jax.random.permutation(stream_key, number_of)
    packed, usual = shares(number_of, rows * top, reach, skew, True), shares(number_of, rows * top, reach, skew, False)
    places = jnp.arange(number_of)

    def named(sizes, offset_by):
        used = int((sizes > 0).sum())
        fixed = max(1, used // 4)
        shifted = fixed + (places - fixed + offset_by * (used - fixed)) % max(1, number_of - fixed)
        return jnp.zeros((number_of,), jnp.int32).at[ranking[jnp.where(places < fixed, places, shifted)]].set(jnp.asarray(sizes, jnp.int32))

    sizes = jnp.where(number % 4 == 0, named(packed, number // 4), named(usual, number - number // 4 - 1))
    mixed = jax.random.permutation(jax.random.fold_in(own, 3), number_of)
    giver, receiver = mixed[0:number_of // 2 * 2:2], mixed[1:number_of // 2 * 2:2]
    margin = jnp.minimum(sizes[giver] - 1, reach - sizes[receiver]) // 2
    margin = jnp.where((giver == ranking[0]) | (receiver == ranking[0]) | (sizes[receiver] == 0), 0, jnp.maximum(margin, 0))
    shifted = jax.random.randint(jax.random.fold_in(own, 4), (number_of // 2,), 0, 1 << 20) % (margin + 1)
    sizes = sizes.at[giver].add(-shifted).at[receiver].add(shifted)
    items = jnp.searchsorted(jnp.cumsum(sizes), jnp.arange(rows * top), side="right").astype(jnp.int32)
    listing = items.reshape(top, rows).T
    listing = listing[jax.random.permutation(jax.random.fold_in(own, 1), rows)]
    offset_by = jax.random.randint(jax.random.fold_in(own, 2), (rows, 1), 0, top)
    return jnp.take_along_axis(listing, (jnp.arange(top)[None, :] + offset_by) % top, axis=1)


def shares(count, total, bound, skew, full):
    weights = [(1 << 20) // math.isqrt(rank ** skew) + 1 for rank in range(1, count + 1)]
    largest = bound if full else min(bound, max(-(-total // count), total * weights[0] // sum(weights)))
    least = 1 if total - largest >= count - 1 else 0
    holding, rest = [largest] + [least] * (count - 1), total - largest - least * (count - 1)
    while rest > 0:
        candidates = [i for i in range(1, count) if holding[i] < largest] or [i for i in range(1, count) if holding[i] < bound]
        pool, left = sum([weights[i] for i in candidates]), rest
        for i in candidates:
            extra = min(bound - holding[i], max(1, left * weights[i] // pool), rest)
            holding[i] = holding[i] + extra
            rest = rest - extra
    return np.array(holding)


def centred(own_key, extent, scale, reach, split=(), kind=jnp.bfloat16):
    entries = scale * jax.random.normal(own_key, extent, jnp.float32)
    if split:
        entries = entries * shard_levels(own_key, extent, split, -0.22, 0.18)
    return jnp.clip(entries, -reach, reach).astype(kind)


def setup_inputs(seed: int = 0) -> dict:
    splits = jax.random.split(jax.random.key(seed), 8)
    tokens = centred(splits[0], (TOKENS, D), 1.0, 6.0, ((0, 32),))
    cotangent = centred(splits[1], (TOKENS, D), 0.05, 0.3984375, ((0, 32),))
    expert_ids_keys = jax.random.split(jax.random.fold_in(splits[2], 1), TOKENS // TOK_DEV)
    expert_ids_turns = jax.random.permutation(jax.random.fold_in(splits[2], 3), TOKENS // TOK_DEV)
    expert_ids = jax.vmap(lambda own, number: routed_block(jax.random.fold_in(splits[2], 2), own, number, TOK_DEV, EXPERTS, TOPK, SLOT, 2))(expert_ids_keys, expert_ids_turns).reshape((TOKENS, TOPK))
    gate_weights = jnp.clip(jnp.exp(math.log(1.0) - 2.9957323 * jax.random.uniform(splits[3], (TOKENS, TOPK), jnp.float32) ** shard_levels(splits[3], (TOKENS, TOPK), ((0, 32),), -0.2, 0.2)), 0.05, 1.0)
    w_gate = centred(splits[4], (EXPERTS, D, FH), D ** -0.5, 0.15625, ((0, 16), (1, 2)))
    w_up = centred(splits[5], (EXPERTS, D, FH), D ** -0.5, 0.15625, ((0, 16), (1, 2)))
    w_down = centred(splits[6], (EXPERTS, D, FH), FH ** -0.5, 0.15625, ((0, 16), (1, 2)))
    return dict(tokens=tokens, cotangent=cotangent, expert_ids=expert_ids, gate_weights=gate_weights, w_gate=w_gate, w_up=w_up, w_down=w_down)


SWISH_SLOPE = 1.702


def expert_pass(packed_x, packed_g, gate_mat, up_mat, down_mat):
    pre_gate = jnp.dot(packed_x, gate_mat, preferred_element_type=jnp.float32)
    pre_up = jnp.dot(packed_x, up_mat, preferred_element_type=jnp.float32)
    sigmoid_part = jax.nn.sigmoid(SWISH_SLOPE * pre_gate)
    value = pre_gate * sigmoid_part
    slope_term = sigmoid_part + SWISH_SLOPE * pre_gate * sigmoid_part * (1.0 - sigmoid_part)
    hidden = (value * (pre_up + 1.0)).astype(jnp.bfloat16)
    expert_out = jnp.dot(hidden, down_mat.T, preferred_element_type=jnp.float32).astype(jnp.bfloat16)
    d_hidden = jnp.dot(packed_g, down_mat, preferred_element_type=jnp.float32)
    grad_down = jnp.dot(packed_g.T, hidden, preferred_element_type=jnp.float32)
    d_gate = (d_hidden * (pre_up + 1.0) * slope_term).astype(jnp.bfloat16)
    d_up = (d_hidden * value).astype(jnp.bfloat16)
    grad_gate = jnp.dot(packed_x.T, d_gate, preferred_element_type=jnp.float32)
    grad_up = jnp.dot(packed_x.T, d_up, preferred_element_type=jnp.float32)
    return expert_out, jnp.stack([grad_gate, grad_up, grad_down]).astype(jnp.bfloat16)


def reference(tokens, cotangent, expert_ids, gate_weights, w_gate, w_up, w_down):
    assigns = TOK_DEV * TOPK
    expert_table = jnp.arange(EXPERTS, dtype=jnp.int32)

    def rank_block(block):
        onehot = (block[:, None] == expert_table[None, :]).astype(jnp.int32)
        local_rank = jnp.sum((jnp.cumsum(onehot, axis=0) - onehot) * onehot, axis=1)
        return local_rank, jnp.sum(onehot, axis=0)

    local_rank, block_counts = lax.map(rank_block, expert_ids.reshape(N_EXPERT * N_DP, assigns))
    local_rank = local_rank.reshape(N_EXPERT, N_DP, assigns)
    block_counts = block_counts.reshape(N_EXPERT, N_DP, EXPERTS)
    offsets = jnp.cumsum(block_counts, axis=0) - block_counts
    group_ids = expert_ids.reshape(N_EXPERT, N_DP, assigns)
    position = jnp.take_along_axis(offsets, group_ids, axis=2) + local_rank
    target = jnp.where(position < CAP, position, CAP).astype(jnp.int32)
    gates = gate_weights.reshape(N_EXPERT, N_DP, assigns)
    token_rows = tokens.reshape(N_EXPERT, N_DP, TOK_DEV, D)
    cot_rows = cotangent.reshape(N_EXPERT, N_DP, TOK_DEV, D)
    inputs = (jnp.swapaxes(group_ids, 0, 1), jnp.swapaxes(target, 0, 1), jnp.swapaxes(gates, 0, 1),
              jnp.swapaxes(token_rows, 0, 1), jnp.swapaxes(cot_rows, 0, 1))

    def run_expert(item):
        return expert_pass(item[0], item[1], item[2], item[3], item[4])

    def per_group(totals, group):
        ids_here, target_here, gates_here, tokens_here, cot_here = group
        token_copies = jnp.repeat(tokens_here, TOPK, axis=1)
        gated = (gates_here[:, :, None] * jnp.repeat(cot_here, TOPK, axis=1).astype(jnp.float32)).astype(jnp.bfloat16)
        packed_x = jnp.zeros((EXPERTS, CAP, D), jnp.bfloat16).at[ids_here, target_here].set(token_copies, mode="drop")
        packed_g = jnp.zeros((EXPERTS, CAP, D), jnp.bfloat16).at[ids_here, target_here].set(gated, mode="drop")
        outputs, group_grads = lax.map(run_expert, (packed_x, packed_g, w_gate, w_up, w_down))
        group_grads = lax.optimization_barrier(group_grads)
        totals = totals + group_grads.astype(jnp.float32)
        kept = (target_here < CAP).astype(jnp.float32)
        fetched = outputs[ids_here, jnp.minimum(target_here, CAP - 1)]
        weighted = (gates_here * kept)[:, :, None] * fetched.astype(jnp.float32)
        mixed_group = jnp.sum(weighted.reshape(N_EXPERT, TOK_DEV, TOPK, D), axis=2).astype(jnp.bfloat16)
        return totals, mixed_group

    totals = jnp.zeros((EXPERTS, 3, D, FH), jnp.float32)
    totals, mixed_all = lax.scan(per_group, totals, inputs)
    mixed = jnp.swapaxes(mixed_all, 0, 1).reshape(TOKENS, D)
    grads = totals.astype(jnp.bfloat16)
    return (mixed, grads[:, 0], grads[:, 1], grads[:, 2])
```

```python
import functools

import jax
import jax.numpy as jnp
from jax import lax
from jax.experimental import pallas as pl
from jax.experimental.pallas import tpu as pltpu
from jax.sharding import PartitionSpec as P

CAP = 512
INNER = 4
SWISH_SLOPE = 1.702
F32 = jnp.float32
BF16 = jnp.bfloat16


def dot(a, b):
    return jnp.dot(a, b, preferred_element_type=F32)


def dot_nt(a, b):
    return lax.dot_general(a, b, (((1,), (1,)), ((), ())), preferred_element_type=F32)


def dot_tn(a, b):
    return lax.dot_general(a, b, (((0,), (0,)), ((), ())), preferred_element_type=F32)


def share_kernel(size, x_ref, all_ref, send_sem, recv_sem):
    me = lax.axis_index("expert")
    barrier = pltpu.get_barrier_semaphore()
    for k in range(1, size):
        pl.semaphore_signal(
            barrier, inc=1, device_id={"expert": lax.rem(me + k, size)},
            device_id_type=pl.DeviceIdType.MESH,
        )
    pl.semaphore_wait(barrier, size - 1)
    copies = []
    for k in range(1, size):
        copy = pltpu.make_async_remote_copy(
            src_ref=x_ref, dst_ref=all_ref.at[me],
            send_sem=send_sem.at[k], recv_sem=recv_sem.at[k],
            device_id={"expert": lax.rem(me + k, size)},
            device_id_type=pl.DeviceIdType.MESH,
        )
        copy.start()
        copies.append(copy)
    all_ref[me] = x_ref[...]
    for copy in copies:
        copy.wait()


def share(x):
    size = lax.axis_size("expert")
    return pl.pallas_call(
        functools.partial(share_kernel, size),
        out_shape=jax.ShapeDtypeStruct((size,) + x.shape, x.dtype),
        in_specs=[pl.BlockSpec(memory_space=pltpu.VMEM)],
        out_specs=pl.BlockSpec(memory_space=pltpu.VMEM),
        scratch_shapes=[
            pltpu.SemaphoreType.DMA((size,)),
            pltpu.SemaphoreType.DMA((size,)),
        ],
        compiler_params=pltpu.CompilerParams(collective_id=0, has_side_effects=True),
    )(x)


def body(tokens, cotangent, expert_ids, gate_weights, w_gate, w_up, w_down):
    size = lax.axis_size("expert")
    rows, top = expert_ids.shape
    width = tokens.shape[1]
    slot = 3 * rows * top // (2 * size)
    inner = min(INNER, size)
    outer = size // inner
    me = lax.axis_index("expert")
    mine_out, mine_in = me // inner, me % inner
    half = outer // 2
    partner = jnp.bitwise_xor(mine_in, jnp.arange(inner, dtype=jnp.int32))

    def shift(x, by):
        pairs = [(d, (d // inner + by) % outer * inner + d % inner) for d in range(size)]
        return lax.ppermute(x, "expert", pairs)

    def gather_outer(x):
        blocks = [x] + [None] * (outer - 1)
        for r in range(1, half + 1):
            if outer > 1:
                blocks[r] = shift(blocks[r - 1], 1)
        for r in range(1, outer - half):
            blocks[outer - r] = shift(blocks[(outer - r + 1) % outer], -1)
        return blocks

    def exchange(blocks):
        moved = list(blocks)
        for d in range(inner - 1, 0, -1):
            pairs = [(e, e // inner * inner + (e % inner ^ d)) for e in range(size)]
            moved[d] = lax.ppermute(blocks[d], "expert", pairs)
        return jnp.concatenate(moved)

    def relay(blocks):
        held = jnp.concatenate(blocks)
        return exchange([dot(part, held).astype(BF16) for part in select])

    meta = jnp.concatenate([expert_ids.T.astype(F32), gate_weights.T], axis=0)
    meta_all = share(meta)
    meta_all, tokens = lax.optimization_barrier((meta_all, tokens))
    token_blocks = gather_outer(tokens)
    token_blocks, cotangent = lax.optimization_barrier((token_blocks, cotangent))
    cot_blocks = gather_outer(cotangent)

    ids_all = meta_all[:, :top, :].astype(jnp.int32)
    gates_all = meta_all[:, top:, :]
    back = (mine_out - jnp.arange(outer, dtype=jnp.int32)) % outer

    before = (jnp.arange(rows)[:, None] < jnp.arange(rows)[None, :]).astype(BF16)

    ids_relay = jnp.stack([
        lax.dynamic_index_in_dim(ids_all, back[r] * inner + mine_in, 0, keepdims=False)
        for r in range(outer)
    ])
    near = mine_out * inner + partner
    named = jnp.any(ids_relay[None] == near[:, None, None, None], axis=2)
    rank = dot(named.astype(BF16).reshape(inner * outer, rows), before)
    rank = rank.reshape(inner, outer, rows).astype(jnp.int32)
    place = jnp.where(named, rank, slot)
    hit = place[:, :, None, :] == jnp.arange(slot, dtype=jnp.int32)[None, None, :, None]
    same = jnp.eye(outer, dtype=jnp.bool_)
    select = (hit[:, :, :, None, :] & same[None, :, None, :, None]).astype(BF16)
    select = select.reshape(inner, outer * slot, outer * rows)

    mask = jnp.any(ids_all == me, axis=1)
    gate_of = jnp.sum(jnp.where(ids_all == me, gates_all, 0.0), axis=1)
    counts = jnp.sum(mask.astype(jnp.int32), axis=1)
    below = jnp.arange(size)[:, None] > jnp.arange(size)[None, :]
    starts = jnp.sum(jnp.where(below, counts[None, :], 0), axis=1)
    own_rank = dot(mask.astype(BF16), before).astype(jnp.int32)
    position = jnp.where(mask, starts[:, None] + own_rank, CAP).reshape(1, size * rows)
    row_index = jnp.arange(CAP, dtype=jnp.int32)
    row_gate = jnp.sum(
        jnp.where(position == row_index[:, None], gate_of.reshape(1, size * rows), 0.0),
        axis=1, keepdims=True,
    )
    source = back[None, :] * inner + partner[:, None]
    is_source = source[:, :, None] == jnp.arange(size, dtype=jnp.int32)
    slot_start = jnp.sum(jnp.where(is_source, starts, 0), axis=2)
    slot_live = jnp.sum(jnp.where(is_source, counts, 0), axis=2)
    within = jnp.arange(slot, dtype=jnp.int32)
    slot_row = jnp.where(
        within < slot_live[:, :, None], slot_start[:, :, None] + within, CAP
    ).reshape(1, inner * outer * slot)
    pack = (row_index[:, None] == slot_row).astype(BF16)

    full_gate, full_up, full_down = (
        lax.all_gather(w_gate, "dp", axis=1, tiled=True)[0],
        lax.all_gather(w_up, "dp", axis=1, tiled=True)[0],
        lax.all_gather(w_down, "dp", axis=1, tiled=True)[0],
    )

    recv_x = relay(token_blocks)
    packed_x = dot(pack, recv_x).astype(BF16)
    pre_gate = dot(packed_x, full_gate)
    pre_up = dot(packed_x, full_up)
    sig = jax.nn.sigmoid(SWISH_SLOPE * pre_gate)
    value = pre_gate * sig
    slope = sig + SWISH_SLOPE * pre_gate * sig * (1.0 - sig)
    hidden = (value * (pre_up + 1.0)).astype(BF16)
    out = (dot_nt(hidden, full_down) * row_gate).astype(BF16)
    spread = dot_tn(pack, out).astype(BF16).reshape(inner, outer * slot, width)

    recv_g = relay(cot_blocks)
    spread, recv_g = lax.optimization_barrier((spread, recv_g))
    returned = exchange([spread[d] for d in range(inner)])
    packed_g = (dot(pack, recv_g) * row_gate).astype(BF16)
    grad_down = dot_tn(packed_g, hidden).astype(BF16)
    d_hidden = dot(packed_g, full_down)
    d_gate = (d_hidden * (pre_up + 1.0) * slope).astype(BF16)
    d_up = (d_hidden * value).astype(BF16)
    returned, grad_down, d_gate, d_up = lax.optimization_barrier(
        (returned, grad_down, d_gate, d_up)
    )
    partial = dot_tn(select.reshape(inner * outer * slot, outer * rows), returned)
    partial = partial.reshape(outer, rows, width)
    partial, d_gate, d_up = lax.optimization_barrier((partial, d_gate, d_up))
    grad_gate = dot_tn(packed_x, d_gate).astype(BF16)
    grad_up = dot_tn(packed_x, d_up).astype(BF16)

    total = partial[0]
    ahead = partial[half]
    behind = partial[half + 1] if outer - half > 1 else None
    for r in range(half - 1, -1, -1):
        ahead = shift(ahead.astype(BF16), -1).astype(F32)
        if r > 0:
            ahead = ahead + partial[r]
    for r in range(half + 2, outer + 1):
        behind = shift(behind.astype(BF16), 1).astype(F32)
        if r < outer:
            behind = behind + partial[r]
    if half > 0:
        total = total + ahead
    if behind is not None:
        total = total + behind
    mixed = total.astype(BF16)

    grads = [
        lax.psum_scatter(g, "dp", scatter_dimension=0, tiled=True)[None]
        for g in (grad_down, grad_gate, grad_up)
    ]
    return mixed, grads[1], grads[2], grads[0]


def solution(mesh):
    rows = P(("expert", "dp"), None)
    mats = P("expert", "dp", None)
    return jax.shard_map(
        body,
        mesh=mesh,
        in_specs=(rows, rows, rows, rows, mats, mats, mats),
        out_specs=(rows, mats, mats, mats),
        check_vma=False,
    )
```

```python
import functools

import jax
import jax.numpy as jnp
from jax import lax
from jax.experimental import pallas as pl
from jax.experimental.pallas import tpu as pltpu
from jax.sharding import PartitionSpec as P


CAP = 512
INNER = 4
SWISH_SLOPE = 1.702
F32 = jnp.float32
BF16 = jnp.bfloat16


def dot(a, b):
    return jnp.dot(a, b, preferred_element_type=F32)


def dot_nt(a, b):
    return lax.dot_general(a, b, (((1,), (1,)), ((), ())), preferred_element_type=F32)


def dot_tn(a, b):
    return lax.dot_general(a, b, (((0,), (0,)), ((), ())), preferred_element_type=F32)


def share_kernel(size, x_ref, all_ref, send_sem, recv_sem):
    me = lax.axis_index("expert")
    barrier = pltpu.get_barrier_semaphore()
    for k in range(1, size):
        pl.semaphore_signal(
            barrier, inc=1, device_id={"expert": lax.rem(me + k, size)},
            device_id_type=pl.DeviceIdType.MESH,
        )
    pl.semaphore_wait(barrier, size - 1)
    copies = []
    for k in range(1, size):
        copy = pltpu.make_async_remote_copy(
            src_ref=x_ref, dst_ref=all_ref.at[me],
            send_sem=send_sem.at[k], recv_sem=recv_sem.at[k],
            device_id={"expert": lax.rem(me + k, size)},
            device_id_type=pl.DeviceIdType.MESH,
        )
        copy.start()
        copies.append(copy)
    all_ref[me] = x_ref[...]
    for copy in copies:
        copy.wait()


def share(x):
    size = lax.axis_size("expert")
    return pl.pallas_call(
        functools.partial(share_kernel, size),
        out_shape=jax.ShapeDtypeStruct((size,) + x.shape, x.dtype),
        in_specs=[pl.BlockSpec(memory_space=pltpu.VMEM)],
        out_specs=pl.BlockSpec(memory_space=pltpu.VMEM),
        scratch_shapes=[
            pltpu.SemaphoreType.DMA((size,)),
            pltpu.SemaphoreType.DMA((size,)),
        ],
        compiler_params=pltpu.CompilerParams(collective_id=0, has_side_effects=True),
    )(x)


def layer(tokens, cotangent, expert_ids, gate_weights, w_gate, w_up, w_down):
    size = lax.axis_size("expert")
    rows, top = expert_ids.shape
    width = tokens.shape[1]
    slot = 3 * rows * top // (2 * size)
    inner = min(INNER, size)
    outer = size // inner
    me = lax.axis_index("expert")
    mine_out, mine_in = me // inner, me % inner
    half = outer // 2
    partner = jnp.bitwise_xor(mine_in, jnp.arange(inner, dtype=jnp.int32))

    def shift(x, by):
        pairs = [(d, (d // inner + by) % outer * inner + d % inner) for d in range(size)]
        return lax.ppermute(x, "expert", pairs)

    def gather_outer(x):
        blocks = [x] + [None] * (outer - 1)
        for r in range(1, half + 1):
            if outer > 1:
                blocks[r] = shift(blocks[r - 1], 1)
        for r in range(1, outer - half):
            blocks[outer - r] = shift(blocks[(outer - r + 1) % outer], -1)
        return blocks

    def exchange(blocks):
        moved = list(blocks)
        for d in range(inner - 1, 0, -1):
            pairs = [(e, e // inner * inner + (e % inner ^ d)) for e in range(size)]
            moved[d] = lax.ppermute(blocks[d], "expert", pairs)
        return jnp.concatenate(moved)

    def relay(blocks):
        held = jnp.concatenate(blocks)
        return exchange([dot(part, held).astype(BF16) for part in select])

    meta = jnp.concatenate([expert_ids.T.astype(F32), gate_weights.T], axis=0)
    meta_all = share(meta)
    meta_all, tokens = lax.optimization_barrier((meta_all, tokens))
    token_blocks = gather_outer(tokens)
    token_blocks, cotangent = lax.optimization_barrier((token_blocks, cotangent))
    cot_blocks = gather_outer(cotangent)

    ids_all = meta_all[:, :top, :].astype(jnp.int32)
    gates_all = meta_all[:, top:, :]
    back = (mine_out - jnp.arange(outer, dtype=jnp.int32)) % outer

    before = (jnp.arange(rows)[:, None] < jnp.arange(rows)[None, :]).astype(BF16)

    ids_relay = jnp.stack([
        lax.dynamic_index_in_dim(ids_all, back[r] * inner + mine_in, 0, keepdims=False)
        for r in range(outer)
    ])
    near = mine_out * inner + partner
    named = jnp.any(ids_relay[None] == near[:, None, None, None], axis=2)
    rank = dot(named.astype(BF16).reshape(inner * outer, rows), before)
    rank = rank.reshape(inner, outer, rows).astype(jnp.int32)
    place = jnp.where(named, rank, slot)
    hit = place[:, :, None, :] == jnp.arange(slot, dtype=jnp.int32)[None, None, :, None]
    same = jnp.eye(outer, dtype=jnp.bool_)
    select = (hit[:, :, :, None, :] & same[None, :, None, :, None]).astype(BF16)
    select = select.reshape(inner, outer * slot, outer * rows)

    mask = jnp.any(ids_all == me, axis=1)
    gate_of = jnp.sum(jnp.where(ids_all == me, gates_all, 0.0), axis=1)
    counts = jnp.sum(mask.astype(jnp.int32), axis=1)
    below = jnp.arange(size)[:, None] > jnp.arange(size)[None, :]
    starts = jnp.sum(jnp.where(below, counts[None, :], 0), axis=1)
    own_rank = dot(mask.astype(BF16), before).astype(jnp.int32)
    position = jnp.where(mask, starts[:, None] + own_rank, CAP).reshape(1, size * rows)
    row_index = jnp.arange(CAP, dtype=jnp.int32)
    row_gate = jnp.sum(
        jnp.where(position == row_index[:, None], gate_of.reshape(1, size * rows), 0.0),
        axis=1, keepdims=True,
    )
    source = back[None, :] * inner + partner[:, None]
    is_source = source[:, :, None] == jnp.arange(size, dtype=jnp.int32)
    slot_start = jnp.sum(jnp.where(is_source, starts, 0), axis=2)
    slot_live = jnp.sum(jnp.where(is_source, counts, 0), axis=2)
    within = jnp.arange(slot, dtype=jnp.int32)
    slot_row = jnp.where(
        within < slot_live[:, :, None], slot_start[:, :, None] + within, CAP
    ).reshape(1, inner * outer * slot)
    pack = (row_index[:, None] == slot_row).astype(BF16)

    full_gate, full_up, full_down = (
        lax.all_gather(w_gate, "dp", axis=1, tiled=True)[0],
        lax.all_gather(w_up, "dp", axis=1, tiled=True)[0],
        lax.all_gather(w_down, "dp", axis=1, tiled=True)[0],
    )

    recv_x = relay(token_blocks)
    packed_x = dot(pack, recv_x).astype(BF16)
    pre_gate = dot(packed_x, full_gate)
    pre_up = dot(packed_x, full_up)
    sig = jax.nn.sigmoid(SWISH_SLOPE * pre_gate)
    value = pre_gate * sig
    slope = sig + SWISH_SLOPE * pre_gate * sig * (1.0 - sig)
    hidden = (value * (pre_up + 1.0)).astype(BF16)
    out = (dot_nt(hidden, full_down) * row_gate).astype(BF16)
    spread = dot_tn(pack, out).astype(BF16).reshape(inner, outer * slot, width)

    recv_g = relay(cot_blocks)
    spread, recv_g = lax.optimization_barrier((spread, recv_g))
    returned = exchange([spread[d] for d in range(inner)])
    packed_g = (dot(pack, recv_g) * row_gate).astype(BF16)
    grad_down = dot_tn(packed_g, hidden).astype(BF16)
    d_hidden = dot(packed_g, full_down)
    d_gate = (d_hidden * (pre_up + 1.0) * slope).astype(BF16)
    d_up = (d_hidden * value).astype(BF16)
    returned, d_gate, d_up = lax.optimization_barrier((returned, d_gate, d_up))
    partial = dot_tn(select.reshape(inner * outer * slot, outer * rows), returned)
    partial = partial.reshape(outer, rows, width)
    partial, d_gate, d_up = lax.optimization_barrier((partial, d_gate, d_up))
    grad_gate = dot_tn(packed_x, d_gate).astype(BF16)
    grad_up = dot_tn(packed_x, d_up).astype(BF16)

    total = partial[0]
    ahead = partial[half]
    behind = partial[half + 1] if outer - half > 1 else None
    for r in range(half - 1, -1, -1):
        ahead = shift(ahead.astype(BF16), -1).astype(F32)
        if r > 0:
            ahead = ahead + partial[r]
    for r in range(half + 2, outer + 1):
        behind = shift(behind.astype(BF16), 1).astype(F32)
        if r < outer:
            behind = behind + partial[r]
    if half > 0:
        total = total + ahead
    if behind is not None:
        total = total + behind
    mixed = total.astype(BF16)

    grads = [
        lax.psum_scatter(g, "dp", scatter_dimension=0, tiled=True)[None]
        for g in (grad_down, grad_gate, grad_up)
    ]
    return mixed, grads[1], grads[2], grads[0]


def solution(mesh):
    rows = P(("expert", "dp"), None)
    mats = P("expert", "dp", None)
    return jax.shard_map(
        layer,
        mesh=mesh,
        in_specs=(rows, rows, rows, rows, mats, mats, mats),
        out_specs=(rows, mats, mats, mats),
        check_vma=False,
    )
```
